32 devices in a mesh: shard: 8 (over z, core), rep: 4 (over y, x).
Axes of the slice: x: 2, y: 2, z: 4, core: 2. Of those that a mesh axis runs over, the one named last changes fastest.
Arguments:
- tokens: bfloat16 [12288, 5120], P(('shard', 'rep')), may hold values from -700 to 700
- norm_gain: float32 [5120], replicated, may hold values from 0.1 to 1.9
- key_bias: float32 [1024], replicated, may hold values from -4 to 4
- key_weight: bfloat16 [8192, 1024], P('shard'), may hold values from -0.078125 to 0.078125
- cotangent: bfloat16 [12288, 1024], P(('shard', 'rep')), may hold values from -40 to 40
- block_slot: int32 [40], replicated, may hold values from 0 to 63, as said below
Outputs:
- projected: bfloat16 [12288, 1024], P(('shard', 'rep'))
- token_grad: bfloat16 [12288, 5120], P(('shard', 'rep'))
- weight_grad: float32 [8192, 1024], P('shard')
- gain_grad: float32 [5120], replicated
- bias_grad: float32 [1024], replicated
The draws below stay inside these ranges and needn't reach their ends.
Inputs may be any that keep to these rules, and one draw needn't show every extreme that they name: Entries are distinct; block b lies on the device of shard with index block_slot[b] // 8, at its local slot block_slot[b] % 8; in every draw some device holds 8 blocks.
All inputs are finite; a program needn't handle non-finite values.
Results may differ from the reference program's by a relative error of at most 0.013.
Values may be sent and summed in bfloat16 or wider, within the bound.
A program may use at most 128 MiB of HBM per device.

```python
import math
import jax
import jax.numpy as jnp
from jax import lax

D = 5120
KVW = 1024
BLK = 128
TOK_DEV = 384
NBLK = 40
CAP = 8
SLOTS = 64
ALL_TOK = 12288
N_SHARD = 8


def draw_tokens(key, part):
    keys = jax.random.split(key, 3)
    row_scale = jnp.exp(jax.random.uniform(keys[0], (ALL_TOK, 1), minval=0.0, maxval=math.log(10.0)))
    col_scale = jnp.exp(jax.random.uniform(keys[1], (1, D), minval=0.0, maxval=math.log(10.0)))
    base = jnp.clip(jax.random.normal(keys[2], (ALL_TOK, D)), -6.0, 6.0)
    return (base * row_scale * col_scale).astype(jnp.bfloat16)


def draw_cotangent(key, part):
    keys = jax.random.split(key, 1)
    position = jnp.arange(ALL_TOK, dtype=jnp.float32)[:, None] / max(ALL_TOK - 1, 1)
    rising = 1.0 + 2.0 * position
    values = jnp.clip(jax.random.normal(keys[0], (ALL_TOK, KVW)), -6.0, 6.0) * rising
    return values.astype(jnp.bfloat16)


def draw_block_slot(key, part):
    keys = jax.random.split(key, 3)
    full_owner = jax.random.randint(keys[0], (), 0, N_SHARD)
    slot_ids = jnp.arange(SLOTS, dtype=jnp.int32)
    order_slots = jax.random.permutation(keys[1], SLOTS).astype(jnp.int32)
    scores = jnp.where(slot_ids // CAP == full_owner, 0, 1 + order_slots)
    chosen = jnp.argsort(scores, stable=True)[:NBLK].astype(jnp.int32)
    block_order = jax.random.permutation(keys[2], NBLK).astype(jnp.int32)
    return chosen[block_order]


def level_of(key, shape, cuts, low, top_value):
    def one(axis_at, shards_of):
        draws = jax.random.uniform(jax.random.fold_in(jax.random.fold_in(key, 6), axis_at), (shards_of,), jnp.float32, low / len(cuts), top_value / len(cuts))
        return jnp.repeat(jnp.exp(draws), shape[axis_at] // shards_of).reshape((-1,) + (1,) * (len(shape) - axis_at - 1))

    factor_of = one(*cuts[0])
    for cut in cuts[1:]:
        factor_of = factor_of * one(*cut)
    return factor_of


def noise(own_key, dims, deviation, bound, pieces=(), held_as=jnp.bfloat16):
    loudness = level_of(own_key, dims, pieces, -0.22, 0.18) if pieces else 1.0
    drawn = jax.random.normal(own_key, dims, jnp.float32) * deviation * loudness
    return jnp.minimum(jnp.maximum(drawn, -bound), bound).astype(held_as)


def setup_inputs(seed: int = 0) -> dict:
    streams_of = jax.random.split(jax.random.key(seed), 7)
    tokens = draw_tokens(jax.random.fold_in(streams_of[6], 71), 0)
    norm_gain = jnp.clip(1.0 + 0.18 * jax.random.normal(streams_of[1], (D,), jnp.float32), 0.1, 1.9)
    key_bias = noise(streams_of[2], (KVW,), 1.0, 4.0, (), jnp.float32)
    key_weight = noise(streams_of[3], (SLOTS * BLK, KVW), D ** -0.5, 0.078125, ((0, 8),))
    cotangent = draw_cotangent(jax.random.fold_in(streams_of[6], 71), 0)
    block_slot = draw_block_slot(jax.random.fold_in(streams_of[6], 71), 0)
    return dict(tokens=tokens, norm_gain=norm_gain, key_bias=key_bias, key_weight=key_weight, cotangent=cotangent, block_slot=block_slot)


EPS = 1e-06

def normalize(tokens, norm_gain):
    values = tokens.astype(jnp.float32)
    inv_rms = lax.rsqrt(lax.optimization_barrier(jnp.mean(values * values, axis=-1, keepdims=True)) + EPS)
    normed = (values * inv_rms * norm_gain).astype(jnp.bfloat16)
    return (values, inv_rms, normed)

def token_backward(values, inv_rms, grad_normed, norm_gain):
    scaled = grad_normed * norm_gain
    inner = lax.optimization_barrier(jnp.mean(scaled * values, axis=-1, keepdims=True))
    return (inv_rms * (scaled - values * inv_rms * inv_rms * inner)).astype(jnp.bfloat16)

def reference(tokens, norm_gain, key_bias, key_weight, cotangent, block_slot):
    whole_weight = key_weight.reshape(SLOTS, BLK, KVW)[block_slot.astype(jnp.int32)].reshape(D, KVW)
    grad_scale = float(ALL_TOK) ** (-0.5)
    device_count = ALL_TOK // TOK_DEV

    def per_device(totals, blocks):
        tok_rows, cot_rows = blocks
        values, inv_rms, normed = normalize(tok_rows, norm_gain)
        forward = jnp.dot(normed, whole_weight, preferred_element_type=jnp.float32)
        projected = (forward + key_bias).astype(jnp.bfloat16)
        grad_normed = lax.dot_general(cot_rows, whole_weight, (((1,), (1,)), ((), ())), preferred_element_type=jnp.float32)
        token_grad = token_backward(values, inv_rms, grad_normed, norm_gain)
        partial_grad = lax.dot_general(normed, cot_rows, (((0,), (0,)), ((), ())), preferred_element_type=jnp.float32) * grad_scale
        rounded = lax.optimization_barrier(partial_grad.astype(jnp.bfloat16)).astype(jnp.float32)
        gain_term = lax.optimization_barrier(jnp.sum(grad_normed * values * inv_rms, axis=0)) * grad_scale
        bias_term = lax.optimization_barrier(jnp.sum(cot_rows.astype(jnp.float32), axis=0)) * grad_scale
        return ((totals[0] + rounded, totals[1] + gain_term, totals[2] + bias_term), (projected, token_grad))
    start = (jnp.zeros((D, KVW), jnp.float32), jnp.zeros((D,), jnp.float32), jnp.zeros((KVW,), jnp.float32))
    totals, outputs = lax.scan(per_device, start, (tokens.reshape(device_count, TOK_DEV, D), cotangent.reshape(device_count, TOK_DEV, KVW)))
    weight_sum, gain_grad, bias_grad = totals
    projected = outputs[0].reshape(ALL_TOK, KVW)
    token_grad = outputs[1].reshape(ALL_TOK, D)
    weight_grad = jnp.zeros((SLOTS, BLK, KVW), jnp.float32).at[block_slot.astype(jnp.int32)].set(weight_sum.reshape(NBLK, BLK, KVW)).reshape(SLOTS * BLK, KVW)
    return (projected, token_grad, weight_grad, gain_grad, bias_grad)
```

```python
import functools
import jax
import jax.numpy as jnp
from jax import lax
from jax.experimental import pallas as pl
from jax.experimental.pallas import tpu as pltpu
from jax.sharding import PartitionSpec as P

BLK = 128
EPS = 1e-06
NJ = 4
SUB = BLK // NJ
QUAD = 4
MESH = pl.DeviceIdType.MESH
F32 = jnp.float32
BF16 = jnp.bfloat16


def comm_kernel(
    planes, cap, nblk, scale,
    tok, gain, cot, bos, w, whole, wgrad,
    inv, part, drecv, r1, r2, slots, zup, zdn, fin, frecv,
    loc_sem, agz_s, agz_r, agx_s, agx_r, agy_s, agy_r, agp_s, agp_r,
    d_s, d_r, r1_s, r1_r, r2_s, r2_r, zu_s, zu_r, zd_s, zd_r, f_s, f_r,
):
    s = lax.axis_index("shard")
    r = lax.axis_index("rep")
    z = s // 2
    c = s % 2
    quad = r % QUAD
    base = r - quad
    y = quad // 2
    x = quad % 2
    xq = y * 2 + (1 - x)
    yq = (1 - y) * 2 + x
    dq = (1 - y) * 2 + (1 - x)
    oc = 1 - c
    partner = (2 * z + oc, r)
    xdev = (s, base + xq)
    ydev = (s, base + yq)
    updev = (s + 2, r)
    dndev = (s - 2, r)
    plane = [(2 * z + oc, r)]
    for q in (xq, yq, dq):
        for cc in (c, oc):
            plane.append((2 * z + cc, base + q))
    has_up = z < planes - 1
    has_dn = z > 0

    bar = pltpu.get_barrier_semaphore()
    for dev in plane:
        pl.semaphore_signal(bar, inc=1, device_id=dev, device_id_type=MESH)

    @pl.when(has_up)
    def _():
        pl.semaphore_signal(bar, inc=1, device_id=updev, device_id_type=MESH)

    @pl.when(has_dn)
    def _():
        pl.semaphore_signal(bar, inc=1, device_id=dndev, device_id_type=MESH)

    pl.semaphore_wait(bar, 7 + has_up.astype(jnp.int32) + has_dn.astype(jnp.int32))

    def rdma(src, dst, ss, rs, dev):
        return pltpu.make_async_remote_copy(
            src_ref=src, dst_ref=dst, send_sem=ss, recv_sem=rs, device_id=dev, device_id_type=MESH
        )

    rows = w.shape[0]
    half = rows // 2
    quar = rows // 4
    hh = (x + y) % 2
    mine = pl.ds(hh * half, half)
    mine_x = pl.ds(hh * half, quar)
    mine_y = pl.ds(hh * half + quar, quar)
    other_x = pl.ds((1 - hh) * half, quar)
    other_y = pl.ds((1 - hh) * half + quar, quar)

    def own_z(d, dev):
        return rdma(w.at[mine], whole.at[s, mine], agz_s.at[d, z], agz_r.at[z], dev)

    def fwd_z(q, d, dev):
        ref = whole.at[2 * q + c, mine]
        return rdma(ref, ref, agz_s.at[d, q], agz_r.at[q], dev)

    def fwd_x(q):
        ref = whole.at[2 * q + c, mine_x]
        return rdma(ref, ref, agx_s.at[q], agx_r.at[q], xdev)

    def fwd_y(q):
        ref = whole.at[2 * q + c, mine_y]
        return rdma(ref, ref, agy_s.at[q], agy_r.at[q], ydev)

    def got_x(q):
        ref = whole.at[2 * q + c, other_x]
        return rdma(ref, ref, agx_s.at[q], agx_r.at[q], xdev)

    def got_y(q):
        ref = whole.at[2 * q + c, other_y]
        return rdma(ref, ref, agy_s.at[q], agy_r.at[q], ydev)

    def to_partner(i, q, rng):
        ref = whole.at[2 * q + c, rng]
        return rdma(ref, ref, agp_s.at[i, q], agp_r.at[i, q], partner)

    def from_partner(i, q, rng):
        ref = whole.at[2 * q + oc, rng]
        return rdma(ref, ref, agp_s.at[i, q], agp_r.at[i, q], partner)

    own_partner = rdma(w, whole.at[s], agp_s.at[0, z], agp_r.at[0, z], partner)
    own_local = pltpu.make_async_copy(w, whole.at[s], loc_sem)

    @pl.when(has_up)
    def _():
        own_z(0, updev).start()

    @pl.when(has_dn)
    def _():
        own_z(1, dndev).start()

    own_partner.start()
    own_local.start()

    def each_foreign(t, f):
        @pl.when(z - t >= 0)
        def _():
            f(z - t, 0)

        @pl.when(z + t < planes)
        def _():
            f(z + t, 1)

    def ag_arrive(t):
        def f(q, d):
            fwd_z(q, d, updev).wait_recv()
            if d == 0:
                @pl.when(has_up)
                def _():
                    fwd_z(q, 0, updev).start()
            else:
                @pl.when(has_dn)
                def _():
                    fwd_z(q, 1, dndev).start()
            fwd_x(q).start()
            fwd_y(q).start()
            to_partner(1, q, mine).start()

        each_foreign(t, f)

    def ag_side(t):
        def f(q, d):
            got_x(q).wait_recv()
            to_partner(2, q, other_x).start()
            got_y(q).wait_recv()
            to_partner(3, q, other_y).start()

        each_foreign(t, f)

    def ag_finish(t):
        def f(q, d):
            from_partner(1, q, mine).wait_recv()
            from_partner(2, q, other_x).wait_recv()
            from_partner(3, q, other_y).wait_recv()
            to_partner(1, q, mine).wait_send()
            to_partner(2, q, other_x).wait_send()
            to_partner(3, q, other_y).wait_send()
            fwd_x(q).wait_send()
            fwd_y(q).wait_send()
            if d == 0:
                @pl.when(has_up)
                def _():
                    fwd_z(q, 0, updev).wait_send()
            else:
                @pl.when(has_dn)
                def _():
                    fwd_z(q, 1, dndev).wait_send()

        each_foreign(t, f)

    tokens_here, width = tok.shape
    wide = 2 * BLK

    def squares(i, acc):
        v = tok[:, pl.ds(pl.multiple_of(i * wide, wide), wide)].astype(F32)
        v = v * v
        return acc + v[:, :BLK] + v[:, BLK:]

    acc = lax.fori_loop(0, width // wide, squares, jnp.zeros((tokens_here, BLK), F32))
    inv[...] = lax.rsqrt(jnp.sum(acc, axis=1, keepdims=True) / width + EPS)

    def term(i, carry):
        cols = pl.ds(pl.multiple_of(i * wide, wide), wide)
        normed = (tok[:, cols].astype(F32) * inv[...] * gain[:, cols]).astype(BF16)
        res = lax.dot_general(
            normed, cot[...], (((0,), (0,)), ((), ())), preferred_element_type=F32
        )
        res = (res * scale).astype(BF16)
        group = res.shape[1] // (2 * QUAD)
        for b in range(2):
            for j in range(NJ):
                lo = b * BLK + j * SUB
                for k in range(QUAD):
                    for cc in range(2):
                        col = (k * 2 + cc) * group
                        part[cc, j, k, i * 2 + b] = res[lo:lo + SUB, col:col + group]
        return carry

    lax.fori_loop(0, nblk // 2, term, 0)

    def d_copy(j):
        return rdma(part.at[oc, j], drecv.at[j], d_s.at[j], d_r.at[j], partner)

    for j in range(NJ):
        d_copy(j).start()

    def add_to(dst, src, count):
        step = 8

        def body(i, carry):
            sl = pl.ds(i * step, step)
            dst[sl] = (dst[sl].astype(F32) + src[sl].astype(F32)).astype(BF16)
            return carry

        lax.fori_loop(0, count // step, body, 0)

    def first_hop(j):
        near, dev = (xq, xdev) if j % 2 == 0 else (yq, ydev)
        return (
            rdma(part.at[c, j, near], r1.at[j, 0], r1_s.at[j, 0], r1_r.at[j, 0], dev),
            rdma(part.at[c, j, dq], r1.at[j, 1], r1_s.at[j, 1], r1_r.at[j, 1], dev),
        )

    def second_hop(j):
        far, dev = (yq, ydev) if j % 2 == 0 else (xq, xdev)
        return rdma(part.at[c, j, far], r2.at[j], r2_s.at[j], r2_r.at[j], dev)

    for j in range(NJ):
        d_copy(j).wait()
        near, far = (xq, yq) if j % 2 == 0 else (yq, xq)
        hops = first_hop(j)
        add_to(part.at[c, j, dq], drecv.at[j, dq], nblk)
        add_to(part.at[c, j, near], drecv.at[j, near], nblk)
        hops[1].start()
        hops[0].start()
        add_to(part.at[c, j, far], drecv.at[j, far], nblk)
        add_to(part.at[c, j, quad], drecv.at[j, quad], nblk)

    ag_arrive(1)
    for j in range(NJ):
        hops = first_hop(j)
        far = yq if j % 2 == 0 else xq
        hops[1].wait_recv()
        add_to(part.at[c, j, far], r1.at[j, 1], nblk)
        second_hop(j).start()
        hops[0].wait_recv()
        add_to(part.at[c, j, quad], r1.at[j, 0], nblk)

    per_plane = 2 * cap

    def z_copy(buf, ss, rs, j, q, dev):
        return rdma(slots.at[j, q], buf.at[j, q], ss.at[j, q], rs.at[j, q], dev)

    def up_copy(j, q):
        return z_copy(zup, zu_s, zu_r, j, q, updev)

    def dn_copy(j, q):
        return z_copy(zdn, zd_s, zd_r, j, q, dndev)

    def place(j):
        second_hop(j).wait_recv()
        add_to(part.at[c, j, quad], r2.at[j], nblk)

        def body(i, carry):
            for u in range(per_plane):
                b = bos[i * per_plane + u]
                val = part[c, j, quad, jnp.maximum(b, 0)]
                slots[j, i, u] = jnp.where(b >= 0, val.astype(F32), 0.0).astype(BF16)
            return carry

        lax.fori_loop(0, planes, body, 0)

    def z_step(j, t):
        qu = planes - 1 - t

        @pl.when(z < qu)
        def _():
            @pl.when(has_dn)
            def _():
                up_copy(j, qu).wait_recv()
                add_to(slots.at[j, qu], zup.at[j, qu], per_plane)

            up_copy(j, qu).start()

        @pl.when(z > t)
        def _():
            @pl.when(has_up)
            def _():
                dn_copy(j, t).wait_recv()
                add_to(slots.at[j, t], zdn.at[j, t], per_plane)

            dn_copy(j, t).start()

    my_id = quad * 2 + c

    def f_copies(j):
        out = []
        for n, dev in enumerate(plane):
            cc = oc if n % 2 == 0 else c
            out.append(
                rdma(
                    fin.at[j, pl.ds(cc * cap, cap)], frecv.at[my_id, j],
                    f_s.at[j, n], f_r.at[j, my_id], dev,
                )
            )
        return out

    def z_end(j):
        @pl.when(has_dn)
        def _():
            up_copy(j, z).wait_recv()
            add_to(slots.at[j, z], zup.at[j, z], per_plane)

        @pl.when(has_up)
        def _():
            dn_copy(j, z).wait_recv()
            add_to(slots.at[j, z], zdn.at[j, z], per_plane)

        fin[j] = slots[j, z]
        frecv[my_id, j] = slots[j, z, pl.ds(c * cap, cap)]
        for cp in f_copies(j):
            cp.start()

    for t in range(2, planes):
        ag_side(t - 1)
        ag_arrive(t)
    for j in range(NJ):
        place(j)
        for t in range(planes - 1):
            z_step(j, t)
    ag_side(planes - 1)
    for j in range(NJ):
        z_end(j)

    def f_got(j, n):
        ids = [quad * 2 + oc]
        for q in (xq, yq, dq):
            ids += [q * 2 + c, q * 2 + oc]
        sender = ids[n]
        return rdma(
            fin.at[j, pl.ds(0, cap)], frecv.at[sender, j],
            f_s.at[j, n], f_r.at[j, sender], plane[n],
        )

    for j in range(NJ):
        for n in range(7):
            f_got(j, n).wait_recv()

        def body(u, carry):
            for n in range(8):
                wgrad[pl.ds(pl.multiple_of(u * BLK + j * SUB, SUB), SUB), n * BLK:(n + 1) * BLK] = (
                    frecv[n, j, u].astype(F32)
                )
            return carry

        lax.fori_loop(0, cap, body, 0)

    for j in range(NJ):
        for cp in first_hop(j):
            cp.wait_send()
        second_hop(j).wait_send()
        for cp in f_copies(j):
            cp.wait_send()
        for t in range(planes - 1):
            @pl.when(z < planes - 1 - t)
            def _():
                up_copy(j, planes - 1 - t).wait_send()

            @pl.when(z > t)
            def _():
                dn_copy(j, t).wait_send()

    for t in range(1, planes):
        ag_finish(t)
    own_partner.wait_send()
    from_partner_own = rdma(w, whole.at[2 * z + oc], agp_s.at[0, z], agp_r.at[0, z], partner)
    from_partner_own.wait_recv()
    own_local.wait()

    @pl.when(has_up)
    def _():
        own_z(0, updev).wait_send()

    @pl.when(has_dn)
    def _():
        own_z(1, dndev).wait_send()


def communicate(tokens, norm_gain, cotangent, block_of_slot, key_weight, scale):
    shard_count = lax.axis_size("shard")
    planes = shard_count // 2
    rows, cols = key_weight.shape
    cap = rows // BLK
    width = tokens.shape[1]
    nblk = width // BLK
    group = cols // (2 * QUAD)
    dma = pltpu.SemaphoreType.DMA
    vm = pltpu.VMEM
    return pl.pallas_call(
        functools.partial(comm_kernel, planes, cap, nblk, scale),
        out_shape=(
            jax.ShapeDtypeStruct((shard_count, rows, cols), BF16),
            jax.ShapeDtypeStruct((rows, cols), F32),
        ),
        in_specs=[
            pl.BlockSpec(memory_space=vm),
            pl.BlockSpec(memory_space=vm),
            pl.BlockSpec(memory_space=vm),
            pl.BlockSpec(memory_space=pltpu.SMEM),
            pl.BlockSpec(memory_space=vm),
        ],
        out_specs=(pl.BlockSpec(memory_space=pl.ANY), pl.BlockSpec(memory_space=vm)),
        scratch_shapes=[
            vm((tokens.shape[0], 1), F32),
            vm((2, NJ, QUAD, nblk, SUB, group), BF16),
            vm((NJ, QUAD, nblk, SUB, group), BF16),
            vm((NJ, 2, nblk, SUB, group), BF16),
            vm((NJ, nblk, SUB, group), BF16),
            vm((NJ, planes, 2 * cap, SUB, group), BF16),
            vm((NJ, planes, 2 * cap, SUB, group), BF16),
            vm((NJ, planes, 2 * cap, SUB, group), BF16),
            vm((NJ, 2 * cap, SUB, group), BF16),
            vm((2 * QUAD, NJ, cap, SUB, group), BF16),
            dma(()),
            dma((2, planes)), dma((planes,)),
            dma((planes,)), dma((planes,)),
            dma((planes,)), dma((planes,)),
            dma((4, planes)), dma((4, planes)),
            dma((NJ,)), dma((NJ,)),
            dma((NJ, 2)), dma((NJ, 2)),
            dma((NJ,)), dma((NJ,)),
            dma((NJ, planes)), dma((NJ, planes)),
            dma((NJ, planes)), dma((NJ, planes)),
            dma((NJ, 7)), dma((NJ, 8)),
        ],
        compiler_params=pltpu.CompilerParams(
            collective_id=0, has_side_effects=True, vmem_limit_bytes=60 * 1024 * 1024
        ),
    )(tokens, norm_gain[None, :], cotangent, block_of_slot, key_weight)


def local(tokens, norm_gain, key_bias, key_weight, cotangent, block_slot):
    row_count, width = tokens.shape
    shard_count = lax.axis_size("shard")
    replicas = lax.axis_size("rep")
    cap = key_weight.shape[0] // BLK
    slot_total = shard_count * cap
    block_count = width // BLK
    grad_scale = float(row_count * shard_count * replicas) ** (-0.5)
    match = block_slot[None, :] == jnp.arange(slot_total, dtype=jnp.int32)[:, None]
    numbers = jnp.arange(1, block_count + 1, dtype=jnp.int32)[None, :]
    block_of_slot = jnp.sum(jnp.where(match, numbers, 0), axis=1) - 1
    whole, weight_grad = communicate(
        tokens, norm_gain, cotangent, block_of_slot, key_weight, grad_scale
    )
    if replicas > QUAD:
        groups = [list(range(i, replicas, QUAD)) for i in range(QUAD)]
        weight_grad = lax.psum(weight_grad, "rep", axis_index_groups=groups)
    weight = jnp.take(whole.reshape(slot_total, BLK, -1), block_slot, axis=0)
    weight = weight.reshape(width, -1)
    values = tokens.astype(F32)
    inv_rms = lax.rsqrt(jnp.mean(values * values, axis=-1, keepdims=True) + EPS)
    normed = (values * inv_rms * norm_gain).astype(BF16)
    projected = jnp.dot(normed, weight, preferred_element_type=F32) + key_bias
    projected = projected.astype(BF16)
    grad_normed = lax.dot_general(
        cotangent, weight, (((1,), (1,)), ((), ())), preferred_element_type=F32
    )
    scaled = grad_normed * norm_gain
    inner = jnp.mean(scaled * values, axis=-1, keepdims=True)
    token_grad = (inv_rms * (scaled - values * inv_rms * inv_rms * inner)).astype(BF16)
    gain_part = jnp.sum(grad_normed * values * inv_rms, axis=0) * grad_scale
    bias_part = jnp.sum(cotangent.astype(F32), axis=0) * grad_scale
    gain_grad, bias_grad = lax.psum((gain_part, bias_part), ("shard", "rep"))
    return (projected, token_grad, weight_grad, gain_grad, bias_grad)


def solution(mesh):
    return jax.shard_map(
        local,
        mesh=mesh,
        in_specs=(
            P(("shard", "rep"), None),
            P(),
            P(),
            P("shard", None),
            P(("shard", "rep"), None),
            P(),
        ),
        out_specs=(
            P(("shard", "rep"), None),
            P(("shard", "rep"), None),
            P("shard", None),
            P(),
            P(),
        ),
        check_vma=False,
    )
```

```python
import functools
import jax
import jax.numpy as jnp
from jax import lax
from jax.experimental import pallas as pl
from jax.experimental.pallas import tpu as pltpu
from jax.sharding import PartitionSpec as P

BLK = 128
EPS = 1e-06
NJ = 4
SUB = BLK // NJ
QUAD = 4
MESH = pl.DeviceIdType.MESH
F32 = jnp.float32
BF16 = jnp.bfloat16


def comm_kernel(
    planes, cap, nblk, scale,
    tok, gain, cot, bias, bos, slot_of, w, proj, tgrad, wgrad, vec,
    whole, inv, coef, fwd, gst, grecv, gz, part, drecv, r1, r2, slots, zup, zdn, fin, frecv,
    loc_sem, agz_s, agz_r, agx_s, agx_r, agy_s, agy_r, agp_s, agp_r,
    d_s, d_r, r1_s, r1_r, r2_s, r2_r, zu_s, zu_r, zd_s, zd_r, f_s, f_r, g_s, g_r, gz_s, gz_r,
):
    s = lax.axis_index("shard")
    r = lax.axis_index("rep")
    z = s // 2
    c = s % 2
    quad = r % QUAD
    base = r - quad
    y = quad // 2
    x = quad % 2
    xq = y * 2 + (1 - x)
    yq = (1 - y) * 2 + x
    dq = (1 - y) * 2 + (1 - x)
    oc = 1 - c
    partner = (2 * z + oc, r)
    xdev = (s, base + xq)
    ydev = (s, base + yq)
    updev = (s + 2, r)
    dndev = (s - 2, r)
    plane = [(2 * z + oc, r)]
    for q in (xq, yq, dq):
        for cc in (c, oc):
            plane.append((2 * z + cc, base + q))
    has_up = z < planes - 1
    has_dn = z > 0

    bar = pltpu.get_barrier_semaphore()
    for dev in plane:
        pl.semaphore_signal(bar, inc=1, device_id=dev, device_id_type=MESH)

    others = [(2 * ((z + d) % planes) + c, r) for d in range(1, planes)]
    for dev in others:
        pl.semaphore_signal(bar, inc=1, device_id=dev, device_id_type=MESH)
    pl.semaphore_wait(bar, 7 + planes - 1)

    def rdma(src, dst, ss, rs, dev):
        return pltpu.make_async_remote_copy(
            src_ref=src, dst_ref=dst, send_sem=ss, recv_sem=rs, device_id=dev, device_id_type=MESH
        )

    half = cap // 2
    quar = cap // 4
    hh = (x + y) % 2

    def span(shard, start, size):
        return whole.at[pl.ds(shard * cap + start, size)]

    mine = (hh * half, half)
    mine_x = (hh * half, quar)
    mine_y = (hh * half + quar, quar)
    other_x = ((1 - hh) * half, quar)
    other_y = ((1 - hh) * half + quar, quar)

    def own_z(d, dev):
        return rdma(w.at[pl.ds(*mine)], span(s, *mine), agz_s.at[d, z], agz_r.at[z], dev)

    def fwd_z(q, d, dev):
        ref = span(2 * q + c, *mine)
        return rdma(ref, ref, agz_s.at[d, q], agz_r.at[q], dev)

    def fwd_x(q):
        ref = span(2 * q + c, *mine_x)
        return rdma(ref, ref, agx_s.at[q], agx_r.at[q], xdev)

    def fwd_y(q):
        ref = span(2 * q + c, *mine_y)
        return rdma(ref, ref, agy_s.at[q], agy_r.at[q], ydev)

    def got_x(q):
        ref = span(2 * q + c, *other_x)
        return rdma(ref, ref, agx_s.at[q], agx_r.at[q], xdev)

    def got_y(q):
        ref = span(2 * q + c, *other_y)
        return rdma(ref, ref, agy_s.at[q], agy_r.at[q], ydev)

    def to_partner(i, q, rng):
        ref = span(2 * q + c, *rng)
        return rdma(ref, ref, agp_s.at[i, q], agp_r.at[i, q], partner)

    def from_partner(i, q, rng):
        ref = span(2 * q + oc, *rng)
        return rdma(ref, ref, agp_s.at[i, q], agp_r.at[i, q], partner)

    own_partner = rdma(w, span(s, 0, cap), agp_s.at[0, z], agp_r.at[0, z], partner)
    own_local = pltpu.make_async_copy(w, span(s, 0, cap), loc_sem)

    @pl.when(has_up)
    def _():
        own_z(0, updev).start()

    @pl.when(has_dn)
    def _():
        own_z(1, dndev).start()

    own_partner.start()
    own_local.start()

    def each_foreign(t, f):
        @pl.when(z - t >= 0)
        def _():
            f(z - t, 0)

        @pl.when(z + t < planes)
        def _():
            f(z + t, 1)

    def ag_arrive(t):
        def f(q, d):
            fwd_z(q, d, updev).wait_recv()
            if d == 0:
                @pl.when(has_up)
                def _():
                    fwd_z(q, 0, updev).start()
            else:
                @pl.when(has_dn)
                def _():
                    fwd_z(q, 1, dndev).start()
            fwd_x(q).start()
            fwd_y(q).start()
            to_partner(1, q, mine).start()

        each_foreign(t, f)

    def ag_side(t):
        def f(q, d):
            got_x(q).wait_recv()
            to_partner(2, q, other_x).start()
            got_y(q).wait_recv()
            to_partner(3, q, other_y).start()

        each_foreign(t, f)

    def ag_finish(t):
        def f(q, d):
            from_partner(1, q, mine).wait_recv()
            from_partner(2, q, other_x).wait_recv()
            from_partner(3, q, other_y).wait_recv()
            to_partner(1, q, mine).wait_send()
            to_partner(2, q, other_x).wait_send()
            to_partner(3, q, other_y).wait_send()
            fwd_x(q).wait_send()
            fwd_y(q).wait_send()
            if d == 0:
                @pl.when(has_up)
                def _():
                    fwd_z(q, 0, updev).wait_send()
            else:
                @pl.when(has_dn)
                def _():
                    fwd_z(q, 1, dndev).wait_send()

        each_foreign(t, f)

    tokens_here, width = tok.shape
    wide = 2 * BLK

    def squares(i, acc):
        v = tok[:, pl.ds(pl.multiple_of(i * wide, wide), wide)].astype(F32)
        v = v * v
        return acc + v[:, :BLK] + v[:, BLK:]

    acc = lax.fori_loop(0, width // wide, squares, jnp.zeros((tokens_here, BLK), F32))
    inv[...] = lax.rsqrt(jnp.sum(acc, axis=1, keepdims=True) / width + EPS)

    def term(i, carry):
        cols = pl.ds(pl.multiple_of(i * wide, wide), wide)
        normed = (tok[:, cols].astype(F32) * inv[...] * gain[:, cols]).astype(BF16)
        res = lax.dot_general(
            normed, cot[...], (((0,), (0,)), ((), ())), preferred_element_type=F32
        )
        res = (res * scale).astype(BF16)
        group = res.shape[1] // (2 * QUAD)
        for b in range(2):
            for j in range(NJ):
                lo = b * BLK + j * SUB
                for k in range(QUAD):
                    for cc in range(2):
                        col = (k * 2 + cc) * group
                        part[cc, j, k, i * 2 + b] = res[lo:lo + SUB, col:col + group]
        return carry


    hb = nblk // 2

    def d_copy(j, i):
        blocks = pl.ds(i * hb, hb)
        return rdma(
            part.at[oc, j, :, blocks], drecv.at[j, :, blocks], d_s.at[j, i], d_r.at[j, i], partner
        )

    for i in range(2):
        lax.fori_loop(i * hb // 2, (i + 1) * hb // 2, term, 0)
        for j in range(NJ):
            d_copy(j, i).start()

    def add_to(dst, src, count):
        step = 8

        def body(i, carry):
            sl = pl.ds(i * step, step)
            dst[sl] = (dst[sl].astype(F32) + src[sl].astype(F32)).astype(BF16)
            return carry

        lax.fori_loop(0, count // step, body, 0)

    def first_hop(j):
        near, dev = (xq, xdev) if j % 2 == 0 else (yq, ydev)
        return (
            rdma(part.at[c, j, near], r1.at[j, 0], r1_s.at[j, 0], r1_r.at[j, 0], dev),
            rdma(part.at[c, j, dq], r1.at[j, 1], r1_s.at[j, 1], r1_r.at[j, 1], dev),
        )

    def second_hop(j):
        far, dev = (yq, ydev) if j % 2 == 0 else (xq, xdev)
        return rdma(part.at[c, j, far], r2.at[j], r2_s.at[j], r2_r.at[j], dev)

    def core_sum(j):
        for i in range(2):
            d_copy(j, i).wait()
        for k in range(QUAD):
            add_to(part.at[c, j, k], drecv.at[j, k], nblk)

    def first_send(j):
        hops = first_hop(j)
        hops[1].start()
        hops[0].start()

    def second_send(j):
        hops = first_hop(j)
        far = yq if j % 2 == 0 else xq
        hops[1].wait_recv()
        add_to(part.at[c, j, far], r1.at[j, 1], nblk)
        second_hop(j).start()
        hops[0].wait_recv()
        add_to(part.at[c, j, quad], r1.at[j, 0], nblk)

    per_plane = 2 * cap

    def z_copy(buf, ss, rs, j, q, dev):
        return rdma(slots.at[j, q], buf.at[j, q], ss.at[j, q], rs.at[j, q], dev)

    def up_copy(j, q):
        return z_copy(zup, zu_s, zu_r, j, q, updev)

    def dn_copy(j, q):
        return z_copy(zdn, zd_s, zd_r, j, q, dndev)

    def place(j):
        second_hop(j).wait_recv()
        add_to(part.at[c, j, quad], r2.at[j], nblk)

        def body(i, carry):
            for u in range(per_plane):
                b = bos[i * per_plane + u]
                val = part[c, j, quad, jnp.maximum(b, 0)]
                slots[j, i, u] = jnp.where(b >= 0, val.astype(F32), 0.0).astype(BF16)
            return carry

        lax.fori_loop(0, planes, body, 0)

    def z_step(j, t):
        qu = planes - 1 - t

        @pl.when(z < qu)
        def _():
            @pl.when(has_dn)
            def _():
                up_copy(j, qu).wait_recv()
                add_to(slots.at[j, qu], zup.at[j, qu], per_plane)

            up_copy(j, qu).start()

        @pl.when(z > t)
        def _():
            @pl.when(has_up)
            def _():
                dn_copy(j, t).wait_recv()
                add_to(slots.at[j, t], zdn.at[j, t], per_plane)

            dn_copy(j, t).start()

    my_id = quad * 2 + c

    def f_copies(j):
        out = []
        for n, dev in enumerate(plane):
            cc = oc if n % 2 == 0 else c
            out.append(
                rdma(
                    fin.at[j, pl.ds(cc * cap, cap)], frecv.at[my_id, j],
                    f_s.at[j, n], f_r.at[j, my_id], dev,
                )
            )
        return out

    def z_end(j):
        @pl.when(has_dn)
        def _():
            up_copy(j, z).wait_recv()
            add_to(slots.at[j, z], zup.at[j, z], per_plane)

        @pl.when(has_up)
        def _():
            dn_copy(j, z).wait_recv()
            add_to(slots.at[j, z], zdn.at[j, z], per_plane)

        fin[j] = slots[j, z]
        frecv[my_id, j] = slots[j, z, pl.ds(c * cap, cap)]
        for cp in f_copies(j):
            cp.start()

    grp = 4
    gw = grp * BLK

    def weight_group(g):
        return jnp.concatenate([whole[slot_of[g * grp + i]] for i in range(grp)], axis=0)

    def fwd_body(g, carry):
        cols = pl.ds(pl.multiple_of(g * gw, gw), gw)
        normed = (tok[:, cols].astype(F32) * inv[...] * gain[:, cols]).astype(BF16)
        fwd[...] += jnp.dot(normed, weight_group(g), preferred_element_type=F32)
        return carry

    def bwd_body(g, carry):
        cols = pl.ds(pl.multiple_of(g * gw, gw), gw)
        grad = lax.dot_general(
            cot[...], weight_group(g), (((1,), (1,)), ((), ())), preferred_element_type=F32
        )
        values = tok[:, cols].astype(F32)
        tgrad[:, cols] = (grad * gain[:, cols] * inv[...] - values * coef[...]).astype(BF16)
        gst[0, :, cols] = jnp.sum(grad * values * inv[...], axis=0, keepdims=True) * scale
        return carry

    groups = nblk // grp
    cuts = [0, groups // 2, groups]

    def fwd_part(i):
        lax.fori_loop(cuts[i], cuts[i + 1], fwd_body, 0)

    def bwd_part(i):
        lax.fori_loop(cuts[i], cuts[i + 1], bwd_body, 0)

    def fwd_end():
        total = fwd[...]
        proj[...] = (total + bias[...]).astype(BF16)
        inner = jnp.sum(total * cot[...].astype(F32), axis=1, keepdims=True) / width
        coef[...] = inv[...] * inv[...] * inner

    def g_copy(n):
        dev = (partner, xdev, ydev)[n]
        return rdma(gst.at[n], grecv.at[n], g_s.at[n], g_r.at[n], dev)

    def g_step(n):
        g_copy(n).wait_recv()
        gst[n + 1] = gst[n] + grecv[n]
        if n < 2:
            g_copy(n + 1).start()

    def gz_copy(d):
        return rdma(gst.at[3], gz.at[z], gz_s.at[d - 1], gz_r.at[z], others[d - 1])

    def gz_got(d):
        q = (z + d) % planes
        return rdma(gst.at[3], gz.at[q], gz_s.at[d - 1], gz_r.at[q], others[d - 1])

    own_local.wait()
    fwd[...] = jnp.zeros_like(fwd)
    gst[0, :, width:] = jnp.sum(cot[...].astype(F32), axis=0, keepdims=True) * scale
    early = list(range(NJ // 2))
    late = list(range(NJ // 2, NJ))
    for j in early:
        core_sum(j)
        first_send(j)
    for j in late:
        core_sum(j)
    ag_arrive(1)
    for j in early:
        second_send(j)
    for j in late:
        first_send(j)
    for t in range(2, planes - 1):
        ag_side(t - 1)
        ag_arrive(t)
    for j in early:
        place(j)
        z_step(j, 0)
    for j in late:
        second_send(j)
    for j in early:
        z_step(j, 1)
    ag_side(planes - 2)
    ag_arrive(planes - 1)
    for j in late:
        place(j)
        z_step(j, 0)
    for t in range(2, planes - 1):
        for j in early:
            z_step(j, t)
    for j in early:
        z_end(j)
    for j in late:
        z_step(j, 1)
    ag_side(planes - 1)
    for t in range(1, planes):
        ag_finish(t)
    own_partner.wait_send()
    rdma(
        w, span(2 * z + oc, 0, cap), agp_s.at[0, z], agp_r.at[0, z], partner
    ).wait_recv()
    fwd_part(0)
    for t in range(2, planes - 1):
        for j in late:
            z_step(j, t)
    fwd_part(1)
    for j in late:
        z_end(j)
    fwd_end()
    bwd_part(0)
    bwd_part(1)
    g_copy(0).start()

    def f_got(j, n):
        ids = [quad * 2 + oc]
        for q in (xq, yq, dq):
            ids += [q * 2 + c, q * 2 + oc]
        sender = ids[n]
        return rdma(
            fin.at[j, pl.ds(0, cap)], frecv.at[sender, j],
            f_s.at[j, n], f_r.at[j, sender], plane[n],
        )

    for j in range(NJ):
        for n in range(7):
            f_got(j, n).wait_recv()

        def body(u, carry):
            for n in range(8):
                wgrad[pl.ds(pl.multiple_of(u * BLK + j * SUB, SUB), SUB), n * BLK:(n + 1) * BLK] = (
                    frecv[n, j, u].astype(F32)
                )
            return carry

        lax.fori_loop(0, cap, body, 0)
        if j < 3:
            g_step(j)
        if j == 2:
            gz[z] = gst[3]
            for d in range(1, planes):
                gz_copy(d).start()

    for d in range(1, planes):
        gz_got(d).wait_recv()
    total = gz[0]
    for q in range(1, planes):
        total = total + gz[q]
    vec[...] = total
    for d in range(1, planes):
        gz_copy(d).wait_send()
    for n in range(3):
        g_copy(n).wait_send()

    for j in range(NJ):
        for cp in first_hop(j):
            cp.wait_send()
        second_hop(j).wait_send()
        for cp in f_copies(j):
            cp.wait_send()
        for t in range(planes - 1):
            @pl.when(z < planes - 1 - t)
            def _():
                up_copy(j, planes - 1 - t).wait_send()

            @pl.when(z > t)
            def _():
                dn_copy(j, t).wait_send()

    @pl.when(has_up)
    def _():
        own_z(0, updev).wait_send()

    @pl.when(has_dn)
    def _():
        own_z(1, dndev).wait_send()


def communicate(tokens, norm_gain, cotangent, key_bias, block_of_slot, block_slot, key_weight, scale):
    shard_count = lax.axis_size("shard")
    planes = shard_count // 2
    rows, cols = key_weight.shape
    cap = rows // BLK
    tok_count, width = tokens.shape
    nblk = width // BLK
    group = cols // (2 * QUAD)
    dma = pltpu.SemaphoreType.DMA
    vm = pltpu.VMEM
    return pl.pallas_call(
        functools.partial(comm_kernel, planes, cap, nblk, scale),
        out_shape=(
            jax.ShapeDtypeStruct((tok_count, cols), BF16),
            jax.ShapeDtypeStruct((tok_count, width), BF16),
            jax.ShapeDtypeStruct((rows, cols), F32),
            jax.ShapeDtypeStruct((1, width + cols), F32),
        ),
        in_specs=[
            pl.BlockSpec(memory_space=vm),
            pl.BlockSpec(memory_space=vm),
            pl.BlockSpec(memory_space=vm),
            pl.BlockSpec(memory_space=vm),
            pl.BlockSpec(memory_space=pltpu.SMEM),
            pl.BlockSpec(memory_space=pltpu.SMEM),
            pl.BlockSpec(memory_space=vm),
        ],
        out_specs=(pl.BlockSpec(memory_space=vm),) * 4,
        scratch_shapes=[
            vm((shard_count * cap, BLK, cols), BF16),
            vm((tok_count, 1), F32),
            vm((tok_count, 1), F32),
            vm((tok_count, cols), F32),
            vm((4, 1, width + cols), F32),
            vm((3, 1, width + cols), F32),
            vm((planes, 1, width + cols), F32),
            vm((2, NJ, QUAD, nblk, SUB, group), BF16),
            vm((NJ, QUAD, nblk, SUB, group), BF16),
            vm((NJ, 2, nblk, SUB, group), BF16),
            vm((NJ, nblk, SUB, group), BF16),
            vm((NJ, planes, 2 * cap, SUB, group), BF16),
            vm((NJ, planes, 2 * cap, SUB, group), BF16),
            vm((NJ, planes, 2 * cap, SUB, group), BF16),
            vm((NJ, 2 * cap, SUB, group), BF16),
            vm((2 * QUAD, NJ, cap, SUB, group), BF16),
            dma(()),
            dma((2, planes)), dma((planes,)),
            dma((planes,)), dma((planes,)),
            dma((planes,)), dma((planes,)),
            dma((4, planes)), dma((4, planes)),
            dma((NJ, 2)), dma((NJ, 2)),
            dma((NJ, 2)), dma((NJ, 2)),
            dma((NJ,)), dma((NJ,)),
            dma((NJ, planes)), dma((NJ, planes)),
            dma((NJ, planes)), dma((NJ, planes)),
            dma((NJ, 7)), dma((NJ, 8)),
            dma((3,)), dma((3,)),
            dma((planes,)), dma((planes,)),
        ],
        compiler_params=pltpu.CompilerParams(
            collective_id=0, has_side_effects=True, vmem_limit_bytes=67043328
        ),
    )(
        tokens, norm_gain[None, :], cotangent, key_bias[None, :], block_of_slot, block_slot,
        key_weight.reshape(cap, BLK, cols),
    )


def local(tokens, norm_gain, key_bias, key_weight, cotangent, block_slot):
    row_count, width = tokens.shape
    shard_count = lax.axis_size("shard")
    replicas = lax.axis_size("rep")
    cap = key_weight.shape[0] // BLK
    slot_total = shard_count * cap
    block_count = width // BLK
    grad_scale = float(row_count * shard_count * replicas) ** (-0.5)
    match = block_slot[None, :] == jnp.arange(slot_total, dtype=jnp.int32)[:, None]
    numbers = jnp.arange(1, block_count + 1, dtype=jnp.int32)[None, :]
    block_of_slot = jnp.sum(jnp.where(match, numbers, 0), axis=1) - 1
    projected, token_grad, weight_grad, vec = communicate(
        tokens, norm_gain, cotangent, key_bias, block_of_slot, block_slot, key_weight, grad_scale
    )
    if replicas > QUAD:
        groups = [list(range(i, replicas, QUAD)) for i in range(QUAD)]
        weight_grad, vec = lax.psum((weight_grad, vec), "rep", axis_index_groups=groups)
    return (projected, token_grad, weight_grad, vec[0, :width], vec[0, width:])


def solution(mesh):
    return jax.shard_map(
        local,
        mesh=mesh,
        in_specs=(
            P(("shard", "rep"), None),
            P(),
            P(),
            P("shard", None),
            P(("shard", "rep"), None),
            P(),
        ),
        out_specs=(
            P(("shard", "rep"), None),
            P(("shard", "rep"), None),
            P("shard", None),
            P(),
            P(),
        ),
        check_vma=False,
    )
```

```python
import functools
import jax
import jax.numpy as jnp
from jax import lax
from jax.experimental import pallas as pl
from jax.experimental.pallas import tpu as pltpu
from jax.sharding import PartitionSpec as P

BLK = 128
EPS = 1e-06
NJ = 4
SUB = BLK // NJ
QUAD = 4
MESH = pl.DeviceIdType.MESH
F32 = jnp.float32
BF16 = jnp.bfloat16


def comm_kernel(
    planes, cap, nblk, scale,
    tok, gain, cot, bias, bos, slot_of, w, proj, tgrad, wgrad, vec,
    whole, inv, coef, fwd, gst, grecv, gz, part, drecv, r1, r2, slots, zup, zdn, fin, frecv,
    loc_sem, agz_s, agz_r, agx_s, agx_r, agy_s, agy_r, agp_s, agp_r,
    d_s, d_r, r1_s, r1_r, r2_s, r2_r, zu_s, zu_r, zd_s, zd_r, f_s, f_r, g_s, g_r, gz_s, gz_r,
):
    s = lax.axis_index("shard")
    r = lax.axis_index("rep")
    z = s // 2
    c = s % 2
    quad = r % QUAD
    base = r - quad
    y = quad // 2
    x = quad % 2
    xq = y * 2 + (1 - x)
    yq = (1 - y) * 2 + x
    dq = (1 - y) * 2 + (1 - x)
    oc = 1 - c
    partner = (2 * z + oc, r)
    xdev = (s, base + xq)
    ydev = (s, base + yq)
    updev = (s + 2, r)
    dndev = (s - 2, r)
    plane = [(2 * z + oc, r)]
    for q in (xq, yq, dq):
        for cc in (c, oc):
            plane.append((2 * z + cc, base + q))
    has_up = z < planes - 1
    has_dn = z > 0

    bar = pltpu.get_barrier_semaphore()
    for dev in plane:
        pl.semaphore_signal(bar, inc=1, device_id=dev, device_id_type=MESH)

    others = [(2 * ((z + d) % planes) + c, r) for d in range(1, planes)]
    for dev in others:
        pl.semaphore_signal(bar, inc=1, device_id=dev, device_id_type=MESH)
    pl.semaphore_wait(bar, 7 + planes - 1)

    def rdma(src, dst, ss, rs, dev):
        return pltpu.make_async_remote_copy(
            src_ref=src, dst_ref=dst, send_sem=ss, recv_sem=rs, device_id=dev, device_id_type=MESH
        )

    half = cap // 2
    quar = cap // 4
    hh = (x + y) % 2

    def span(shard, start, size):
        return whole.at[pl.ds(shard * cap + start, size)]

    mine = (hh * half, half)
    mine_x = (hh * half, quar)
    mine_y = (hh * half + quar, quar)
    other_x = ((1 - hh) * half, quar)
    other_y = ((1 - hh) * half + quar, quar)

    piece = (mine_x, mine_y)

    def own_z(d, i, dev):
        return rdma(
            w.at[pl.ds(*piece[i])], span(s, *piece[i]), agz_s.at[d, i, z], agz_r.at[i, z], dev
        )

    def fwd_z(q, d, i, dev):
        ref = span(2 * q + c, *piece[i])
        return rdma(ref, ref, agz_s.at[d, i, q], agz_r.at[i, q], dev)

    def fwd_x(q):
        ref = span(2 * q + c, *mine_x)
        return rdma(ref, ref, agx_s.at[q], agx_r.at[q], xdev)

    def fwd_y(q):
        ref = span(2 * q + c, *mine_y)
        return rdma(ref, ref, agy_s.at[q], agy_r.at[q], ydev)

    def got_x(q):
        ref = span(2 * q + c, *other_x)
        return rdma(ref, ref, agx_s.at[q], agx_r.at[q], xdev)

    def got_y(q):
        ref = span(2 * q + c, *other_y)
        return rdma(ref, ref, agy_s.at[q], agy_r.at[q], ydev)

    def to_partner(i, q, rng):
        ref = span(2 * q + c, *rng)
        return rdma(ref, ref, agp_s.at[i, q], agp_r.at[i, q], partner)

    def from_partner(i, q, rng):
        ref = span(2 * q + oc, *rng)
        return rdma(ref, ref, agp_s.at[i, q], agp_r.at[i, q], partner)

    own_partner = rdma(w, span(s, 0, cap), agp_s.at[0, z], agp_r.at[0, z], partner)
    own_local = pltpu.make_async_copy(w, span(s, 0, cap), loc_sem)

    @pl.when(has_up)
    def _():
        own_z(0, 0, updev).start()
        own_z(0, 1, updev).start()

    @pl.when(has_dn)
    def _():
        own_z(1, 0, dndev).start()
        own_z(1, 1, dndev).start()

    own_partner.start()
    own_local.start()

    def each_foreign(t, f):
        @pl.when(z - t >= 0)
        def _():
            f(z - t, 0)

        @pl.when(z + t < planes)
        def _():
            f(z + t, 1)

    def ag_piece(t, i):
        def f(q, d):
            fwd_z(q, d, i, updev).wait_recv()
            if d == 0:
                @pl.when(has_up)
                def _():
                    fwd_z(q, 0, i, updev).start()
            else:
                @pl.when(has_dn)
                def _():
                    fwd_z(q, 1, i, dndev).start()
            if i == 0:
                fwd_x(q).start()
            else:
                fwd_y(q).start()
                to_partner(1, q, mine).start()

        each_foreign(t, f)

    def ag_arrive(t):
        ag_piece(t, 0)
        ag_piece(t, 1)

    def ag_side(t):
        def f(q, d):
            got_x(q).wait_recv()
            to_partner(2, q, other_x).start()
            got_y(q).wait_recv()
            to_partner(3, q, other_y).start()

        each_foreign(t, f)

    def ag_finish(t):
        def f(q, d):
            from_partner(1, q, mine).wait_recv()
            from_partner(2, q, other_x).wait_recv()
            from_partner(3, q, other_y).wait_recv()
            to_partner(1, q, mine).wait_send()
            to_partner(2, q, other_x).wait_send()
            to_partner(3, q, other_y).wait_send()
            fwd_x(q).wait_send()
            fwd_y(q).wait_send()
            if d == 0:
                @pl.when(has_up)
                def _():
                    fwd_z(q, 0, 0, updev).wait_send()
                    fwd_z(q, 0, 1, updev).wait_send()
            else:
                @pl.when(has_dn)
                def _():
                    fwd_z(q, 1, 0, dndev).wait_send()
                    fwd_z(q, 1, 1, dndev).wait_send()

        each_foreign(t, f)

    tokens_here, width = tok.shape
    wide = 2 * BLK

    def squares(i, acc):
        v = tok[:, pl.ds(pl.multiple_of(i * wide, wide), wide)].astype(F32)
        v = v * v
        return acc + v[:, :BLK] + v[:, BLK:]

    acc = lax.fori_loop(0, width // wide, squares, jnp.zeros((tokens_here, BLK), F32))
    inv[...] = lax.rsqrt(jnp.sum(acc, axis=1, keepdims=True) / width + EPS)

    def term(i, carry):
        cols = pl.ds(pl.multiple_of(i * wide, wide), wide)
        normed = (tok[:, cols].astype(F32) * inv[...] * gain[:, cols]).astype(BF16)
        res = lax.dot_general(
            normed, cot[...], (((0,), (0,)), ((), ())), preferred_element_type=F32
        )
        res = (res * scale).astype(BF16)
        group = res.shape[1] // (2 * QUAD)
        for b in range(2):
            for j in range(NJ):
                lo = b * BLK + j * SUB
                for k in range(QUAD):
                    for cc in range(2):
                        col = (k * 2 + cc) * group
                        part[cc, j, k, i * 2 + b] = res[lo:lo + SUB, col:col + group]
        return carry


    hb = nblk // 2

    def d_copy(j, i):
        blocks = pl.ds(i * hb, hb)
        return rdma(
            part.at[oc, j, :, blocks], drecv.at[j, :, blocks], d_s.at[j, i], d_r.at[j, i], partner
        )

    for i in range(2):
        lax.fori_loop(i * hb // 2, (i + 1) * hb // 2, term, 0)
        for j in range(NJ):
            d_copy(j, i).start()
        ag_piece(1, i)

    def add_to(dst, src, count):
        step = 8

        def body(i, carry):
            sl = pl.ds(i * step, step)
            dst[sl] = (dst[sl].astype(F32) + src[sl].astype(F32)).astype(BF16)
            return carry

        lax.fori_loop(0, count // step, body, 0)

    def first_hop(j):
        near, dev = (xq, xdev) if j % 2 == 0 else (yq, ydev)
        return (
            rdma(part.at[c, j, near], r1.at[j, 0], r1_s.at[j, 0], r1_r.at[j, 0], dev),
            rdma(part.at[c, j, dq], r1.at[j, 1], r1_s.at[j, 1], r1_r.at[j, 1], dev),
        )

    def second_hop(j):
        far, dev = (yq, ydev) if j % 2 == 0 else (xq, xdev)
        return rdma(part.at[c, j, far], r2.at[j], r2_s.at[j], r2_r.at[j], dev)

    def core_sum(j):
        for i in range(2):
            d_copy(j, i).wait()
        for k in range(QUAD):
            add_to(part.at[c, j, k], drecv.at[j, k], nblk)

    def first_send(j):
        hops = first_hop(j)
        hops[1].start()
        hops[0].start()

    def second_send(j):
        hops = first_hop(j)
        far = yq if j % 2 == 0 else xq
        hops[1].wait_recv()
        add_to(part.at[c, j, far], r1.at[j, 1], nblk)
        second_hop(j).start()
        hops[0].wait_recv()
        add_to(part.at[c, j, quad], r1.at[j, 0], nblk)

    per_plane = 2 * cap

    def z_copy(buf, ss, rs, j, q, dev):
        return rdma(slots.at[j, q], buf.at[j, q], ss.at[j, q], rs.at[j, q], dev)

    def up_copy(j, q):
        return z_copy(zup, zu_s, zu_r, j, q, updev)

    def dn_copy(j, q):
        return z_copy(zdn, zd_s, zd_r, j, q, dndev)

    def place(j):
        second_hop(j).wait_recv()
        add_to(part.at[c, j, quad], r2.at[j], nblk)

        def body(i, carry):
            for u in range(per_plane):
                b = bos[i * per_plane + u]
                val = part[c, j, quad, jnp.maximum(b, 0)]
                slots[j, i, u] = jnp.where(b >= 0, val.astype(F32), 0.0).astype(BF16)
            return carry

        lax.fori_loop(0, planes, body, 0)

    def z_start(j):
        @pl.when(z == 0)
        def _():
            for q in range(planes - 1, 0, -1):
                up_copy(j, q).start()

        @pl.when(z == planes - 1)
        def _():
            for q in range(planes - 1):
                dn_copy(j, q).start()

    def z_step(j, t):
        qu = planes - 1 - t

        @pl.when(has_dn & (z < qu))
        def _():
            up_copy(j, qu).wait_recv()
            add_to(slots.at[j, qu], zup.at[j, qu], per_plane)
            up_copy(j, qu).start()

        @pl.when(has_up & (z > t))
        def _():
            dn_copy(j, t).wait_recv()
            add_to(slots.at[j, t], zdn.at[j, t], per_plane)
            dn_copy(j, t).start()

    my_id = quad * 2 + c

    def f_copies(j):
        out = []
        for n, dev in enumerate(plane):
            cc = oc if n % 2 == 0 else c
            out.append(
                rdma(
                    fin.at[j, pl.ds(cc * cap, cap)], frecv.at[my_id, j],
                    f_s.at[j, n], f_r.at[j, my_id], dev,
                )
            )
        return out

    def z_end(j):
        @pl.when(has_dn)
        def _():
            up_copy(j, z).wait_recv()
            add_to(slots.at[j, z], zup.at[j, z], per_plane)

        @pl.when(has_up)
        def _():
            dn_copy(j, z).wait_recv()
            add_to(slots.at[j, z], zdn.at[j, z], per_plane)

        fin[j] = slots[j, z]
        frecv[my_id, j] = slots[j, z, pl.ds(c * cap, cap)]
        for cp in f_copies(j):
            cp.start()

    grp = 4
    gw = grp * BLK

    def weight_group(g):
        return jnp.concatenate([whole[slot_of[g * grp + i]] for i in range(grp)], axis=0)

    def fwd_body(g, carry):
        cols = pl.ds(pl.multiple_of(g * gw, gw), gw)
        normed = (tok[:, cols].astype(F32) * inv[...] * gain[:, cols]).astype(BF16)
        fwd[...] += jnp.dot(normed, weight_group(g), preferred_element_type=F32)
        return carry

    def bwd_body(g, carry):
        cols = pl.ds(pl.multiple_of(g * gw, gw), gw)
        grad = lax.dot_general(
            cot[...], weight_group(g), (((1,), (1,)), ((), ())), preferred_element_type=F32
        )
        values = tok[:, cols].astype(F32)
        tgrad[:, cols] = (grad * gain[:, cols] * inv[...] - values * coef[...]).astype(BF16)
        gst[0, :, cols] = jnp.sum(grad * values * inv[...], axis=0, keepdims=True) * scale
        return carry

    groups = nblk // grp
    cuts = [0, groups // 2, groups]

    def fwd_part(i):
        lax.fori_loop(cuts[i], cuts[i + 1], fwd_body, 0)

    def bwd_part(i):
        lax.fori_loop(cuts[i], cuts[i + 1], bwd_body, 0)

    def fwd_end():
        total = fwd[...]
        proj[...] = (total + bias[...]).astype(BF16)
        inner = jnp.sum(total * cot[...].astype(F32), axis=1, keepdims=True) / width
        coef[...] = inv[...] * inv[...] * inner

    def g_copy(n):
        dev = (partner, xdev, ydev)[n]
        return rdma(gst.at[n], grecv.at[n], g_s.at[n], g_r.at[n], dev)

    def g_step(n):
        g_copy(n).wait_recv()
        gst[n + 1] = gst[n] + grecv[n]
        if n < 2:
            g_copy(n + 1).start()

    def gz_copy(d):
        return rdma(gst.at[3], gz.at[z], gz_s.at[d - 1], gz_r.at[z], others[d - 1])

    def gz_got(d):
        q = (z + d) % planes
        return rdma(gst.at[3], gz.at[q], gz_s.at[d - 1], gz_r.at[q], others[d - 1])

    own_local.wait()
    fwd[...] = jnp.zeros_like(fwd)
    gst[0, :, width:] = jnp.sum(cot[...].astype(F32), axis=0, keepdims=True) * scale
    early = list(range(NJ // 2))
    late = list(range(NJ // 2, NJ))
    for j in early:
        core_sum(j)
        first_send(j)
    for j in late:
        core_sum(j)
    for j in early:
        second_send(j)
    for j in late:
        first_send(j)
    for t in range(2, planes - 1):
        ag_side(t - 1)
        ag_arrive(t)
    for j in early:
        place(j)
        z_start(j)
    for j in early:
        z_step(j, 0)
    for j in late:
        second_send(j)
    for j in early:
        z_step(j, 1)
    ag_side(planes - 2)
    ag_arrive(planes - 1)
    for t in range(2, planes - 1):
        for j in early:
            z_step(j, t)
    for j in late:
        place(j)
        z_start(j)
    for j in early:
        z_end(j)
    for t in range(2):
        for j in late:
            z_step(j, t)
    ag_side(planes - 1)
    for t in range(1, planes):
        ag_finish(t)
    own_partner.wait_send()
    rdma(
        w, span(2 * z + oc, 0, cap), agp_s.at[0, z], agp_r.at[0, z], partner
    ).wait_recv()
    fwd_part(0)
    for t in range(2, planes - 1):
        for j in late:
            z_step(j, t)
    for j in late:
        z_end(j)
    fwd_part(1)
    fwd_end()
    bwd_part(0)
    bwd_part(1)
    g_copy(0).start()

    def f_got(j, n):
        ids = [quad * 2 + oc]
        for q in (xq, yq, dq):
            ids += [q * 2 + c, q * 2 + oc]
        sender = ids[n]
        return rdma(
            fin.at[j, pl.ds(0, cap)], frecv.at[sender, j],
            f_s.at[j, n], f_r.at[j, sender], plane[n],
        )

    for j in range(NJ):
        for n in range(7):
            f_got(j, n).wait_recv()

        def body(u, carry):
            for n in range(8):
                wgrad[pl.ds(pl.multiple_of(u * BLK + j * SUB, SUB), SUB), n * BLK:(n + 1) * BLK] = (
                    frecv[n, j, u].astype(F32)
                )
            return carry

        lax.fori_loop(0, cap, body, 0)
        if j < 3:
            g_step(j)
        if j == 2:
            gz[z] = gst[3]
            for d in range(1, planes):
                gz_copy(d).start()

    for d in range(1, planes):
        gz_got(d).wait_recv()
    total = gz[0]
    for q in range(1, planes):
        total = total + gz[q]
    vec[...] = total
    for d in range(1, planes):
        gz_copy(d).wait_send()
    for n in range(3):
        g_copy(n).wait_send()

    for j in range(NJ):
        for cp in first_hop(j):
            cp.wait_send()
        second_hop(j).wait_send()
        for cp in f_copies(j):
            cp.wait_send()
        for t in range(planes - 1):
            @pl.when(z < planes - 1 - t)
            def _():
                up_copy(j, planes - 1 - t).wait_send()

            @pl.when(z > t)
            def _():
                dn_copy(j, t).wait_send()

    @pl.when(has_up)
    def _():
        own_z(0, 0, updev).wait_send()
        own_z(0, 1, updev).wait_send()

    @pl.when(has_dn)
    def _():
        own_z(1, 0, dndev).wait_send()
        own_z(1, 1, dndev).wait_send()


def communicate(tokens, norm_gain, cotangent, key_bias, block_of_slot, block_slot, key_weight, scale):
    shard_count = lax.axis_size("shard")
    planes = shard_count // 2
    rows, cols = key_weight.shape
    cap = rows // BLK
    tok_count, width = tokens.shape
    nblk = width // BLK
    group = cols // (2 * QUAD)
    dma = pltpu.SemaphoreType.DMA
    vm = pltpu.VMEM
    return pl.pallas_call(
        functools.partial(comm_kernel, planes, cap, nblk, scale),
        out_shape=(
            jax.ShapeDtypeStruct((tok_count, cols), BF16),
            jax.ShapeDtypeStruct((tok_count, width), BF16),
            jax.ShapeDtypeStruct((rows, cols), F32),
            jax.ShapeDtypeStruct((1, width + cols), F32),
        ),
        in_specs=[
            pl.BlockSpec(memory_space=vm),
            pl.BlockSpec(memory_space=vm),
            pl.BlockSpec(memory_space=vm),
            pl.BlockSpec(memory_space=vm),
            pl.BlockSpec(memory_space=pltpu.SMEM),
            pl.BlockSpec(memory_space=pltpu.SMEM),
            pl.BlockSpec(memory_space=vm),
        ],
        out_specs=(pl.BlockSpec(memory_space=vm),) * 4,
        scratch_shapes=[
            vm((shard_count * cap, BLK, cols), BF16),
            vm((tok_count, 1), F32),
            vm((tok_count, 1), F32),
            vm((tok_count, cols), F32),
            vm((4, 1, width + cols), F32),
            vm((3, 1, width + cols), F32),
            vm((planes, 1, width + cols), F32),
            vm((2, NJ, QUAD, nblk, SUB, group), BF16),
            vm((NJ, QUAD, nblk, SUB, group), BF16),
            vm((NJ, 2, nblk, SUB, group), BF16),
            vm((NJ, nblk, SUB, group), BF16),
            vm((NJ, planes, 2 * cap, SUB, group), BF16),
            vm((NJ, planes, 2 * cap, SUB, group), BF16),
            vm((NJ, planes, 2 * cap, SUB, group), BF16),
            vm((NJ, 2 * cap, SUB, group), BF16),
            vm((2 * QUAD, NJ, cap, SUB, group), BF16),
            dma(()),
            dma((2, 2, planes)), dma((2, planes)),
            dma((planes,)), dma((planes,)),
            dma((planes,)), dma((planes,)),
            dma((4, planes)), dma((4, planes)),
            dma((NJ, 2)), dma((NJ, 2)),
            dma((NJ, 2)), dma((NJ, 2)),
            dma((NJ,)), dma((NJ,)),
            dma((NJ, planes)), dma((NJ, planes)),
            dma((NJ, planes)), dma((NJ, planes)),
            dma((NJ, 7)), dma((NJ, 8)),
            dma((3,)), dma((3,)),
            dma((planes,)), dma((planes,)),
        ],
        compiler_params=pltpu.CompilerParams(
            collective_id=0, has_side_effects=True, vmem_limit_bytes=67043328
        ),
    )(
        tokens, norm_gain[None, :], cotangent, key_bias[None, :], block_of_slot, block_slot,
        key_weight.reshape(cap, BLK, cols),
    )


def local(tokens, norm_gain, key_bias, key_weight, cotangent, block_slot):
    row_count, width = tokens.shape
    shard_count = lax.axis_size("shard")
    replicas = lax.axis_size("rep")
    cap = key_weight.shape[0] // BLK
    slot_total = shard_count * cap
    block_count = width // BLK
    grad_scale = float(row_count * shard_count * replicas) ** (-0.5)
    match = block_slot[None, :] == jnp.arange(slot_total, dtype=jnp.int32)[:, None]
    numbers = jnp.arange(1, block_count + 1, dtype=jnp.int32)[None, :]
    block_of_slot = jnp.sum(jnp.where(match, numbers, 0), axis=1) - 1
    projected, token_grad, weight_grad, vec = communicate(
        tokens, norm_gain, cotangent, key_bias, block_of_slot, block_slot, key_weight, grad_scale
    )
    if replicas > QUAD:
        groups = [list(range(i, replicas, QUAD)) for i in range(QUAD)]
        weight_grad, vec = lax.psum((weight_grad, vec), "rep", axis_index_groups=groups)
    return (projected, token_grad, weight_grad, vec[0, :width], vec[0, width:])


def solution(mesh):
    return jax.shard_map(
        local,
        mesh=mesh,
        in_specs=(
            P(("shard", "rep"), None),
            P(),
            P(),
            P("shard", None),
            P(("shard", "rep"), None),
            P(),
        ),
        out_specs=(
            P(("shard", "rep"), None),
            P(("shard", "rep"), None),
            P("shard", None),
            P(),
            P(),
        ),
        check_vma=False,
    )
```

```python
import functools
import jax
import jax.numpy as jnp
from jax import lax
from jax.experimental import pallas as pl
from jax.experimental.pallas import tpu as pltpu
from jax.sharding import PartitionSpec as P

BLK = 128
EPS = 1e-06
NJ = 4
SUB = BLK // NJ
QUAD = 4
MESH = pl.DeviceIdType.MESH
F32 = jnp.float32
BF16 = jnp.bfloat16


def comm_kernel(
    planes, cap, nblk, scale,
    tok, gain, cot, bias, bos, slot_of, w, proj, tgrad, wgrad, vec,
    whole, inv, coef, fwd, gst, grecv, gz, part, drecv, r1, r2, slots, zup, zdn, fin, frecv,
    loc_sem, agz_s, agz_r, agx_s, agx_r, agy_s, agy_r, agp_s, agp_r,
    d_s, d_r, r1_s, r1_r, r2_s, r2_r, zu_s, zu_r, zd_s, zd_r, f_s, f_r, g_s, g_r, gz_s, gz_r,
):
    s = lax.axis_index("shard")
    r = lax.axis_index("rep")
    z = s // 2
    c = s % 2
    quad = r % QUAD
    base = r - quad
    y = quad // 2
    x = quad % 2
    xq = y * 2 + (1 - x)
    yq = (1 - y) * 2 + x
    dq = (1 - y) * 2 + (1 - x)
    oc = 1 - c
    partner = (2 * z + oc, r)
    xdev = (s, base + xq)
    ydev = (s, base + yq)
    updev = (s + 2, r)
    dndev = (s - 2, r)
    plane = [(2 * z + oc, r)]
    for q in (xq, yq, dq):
        for cc in (c, oc):
            plane.append((2 * z + cc, base + q))
    has_up = z < planes - 1
    has_dn = z > 0

    bar = pltpu.get_barrier_semaphore()
    for dev in plane:
        pl.semaphore_signal(bar, inc=1, device_id=dev, device_id_type=MESH)

    others = [(2 * ((z + d) % planes) + c, r) for d in range(1, planes)]
    for dev in others:
        pl.semaphore_signal(bar, inc=1, device_id=dev, device_id_type=MESH)
    pl.semaphore_wait(bar, 7 + planes - 1)

    def rdma(src, dst, ss, rs, dev):
        return pltpu.make_async_remote_copy(
            src_ref=src, dst_ref=dst, send_sem=ss, recv_sem=rs, device_id=dev, device_id_type=MESH
        )

    half = cap // 2
    quar = cap // 4
    hh = (x + y) % 2

    def span(shard, start, size):
        return whole.at[pl.ds(shard * cap + start, size)]

    mine = (hh * half, half)
    mine_x = (hh * half, quar)
    mine_y = (hh * half + quar, quar)
    other_x = ((1 - hh) * half, quar)
    other_y = ((1 - hh) * half + quar, quar)

    def own_z(d, dev):
        return rdma(w.at[pl.ds(*mine)], span(s, *mine), agz_s.at[d, z], agz_r.at[z], dev)

    def fwd_z(q, d, dev):
        ref = span(2 * q + c, *mine)
        return rdma(ref, ref, agz_s.at[d, q], agz_r.at[q], dev)

    def fwd_x(q):
        ref = span(2 * q + c, *mine_x)
        return rdma(ref, ref, agx_s.at[q], agx_r.at[q], xdev)

    def fwd_y(q):
        ref = span(2 * q + c, *mine_y)
        return rdma(ref, ref, agy_s.at[q], agy_r.at[q], ydev)

    def got_x(q):
        ref = span(2 * q + c, *other_x)
        return rdma(ref, ref, agx_s.at[q], agx_r.at[q], xdev)

    def got_y(q):
        ref = span(2 * q + c, *other_y)
        return rdma(ref, ref, agy_s.at[q], agy_r.at[q], ydev)

    def to_partner(i, q, rng):
        ref = span(2 * q + c, *rng)
        return rdma(ref, ref, agp_s.at[i, q], agp_r.at[i, q], partner)

    def from_partner(i, q, rng):
        ref = span(2 * q + oc, *rng)
        return rdma(ref, ref, agp_s.at[i, q], agp_r.at[i, q], partner)

    own_partner = rdma(w, span(s, 0, cap), agp_s.at[0, z], agp_r.at[0, z], partner)
    own_local = pltpu.make_async_copy(w, span(s, 0, cap), loc_sem)

    @pl.when(has_up)
    def _():
        own_z(0, updev).start()

    @pl.when(has_dn)
    def _():
        own_z(1, dndev).start()

    own_partner.start()
    own_local.start()

    def each_foreign(t, f):
        @pl.when(z - t >= 0)
        def _():
            f(z - t, 0)

        @pl.when(z + t < planes)
        def _():
            f(z + t, 1)

    def ag_arrive(t):
        def f(q, d):
            fwd_z(q, d, updev).wait_recv()
            if d == 0:
                @pl.when(has_up)
                def _():
                    fwd_z(q, 0, updev).start()
            else:
                @pl.when(has_dn)
                def _():
                    fwd_z(q, 1, dndev).start()
            fwd_x(q).start()
            fwd_y(q).start()
            to_partner(1, q, mine).start()

        each_foreign(t, f)

    def ag_side(t):
        def f(q, d):
            got_x(q).wait_recv()
            to_partner(2, q, other_x).start()
            got_y(q).wait_recv()
            to_partner(3, q, other_y).start()

        each_foreign(t, f)

    def ag_finish(t):
        def f(q, d):
            from_partner(1, q, mine).wait_recv()
            from_partner(2, q, other_x).wait_recv()
            from_partner(3, q, other_y).wait_recv()

        each_foreign(t, f)

    def ag_drain(t):
        def f(q, d):
            to_partner(1, q, mine).wait_send()
            to_partner(2, q, other_x).wait_send()
            to_partner(3, q, other_y).wait_send()
            fwd_x(q).wait_send()
            fwd_y(q).wait_send()
            if d == 0:
                @pl.when(has_up)
                def _():
                    fwd_z(q, 0, updev).wait_send()
            else:
                @pl.when(has_dn)
                def _():
                    fwd_z(q, 1, dndev).wait_send()

        each_foreign(t, f)

    tokens_here, width = tok.shape
    wide = 2 * BLK

    def squares(i, acc):
        v = tok[:, pl.ds(pl.multiple_of(i * wide, wide), wide)].astype(F32)
        v = v * v
        return acc + v[:, :BLK] + v[:, BLK:]

    acc = lax.fori_loop(0, width // wide, squares, jnp.zeros((tokens_here, BLK), F32))
    inv[...] = lax.rsqrt(jnp.sum(acc, axis=1, keepdims=True) / width + EPS)

    def term(i, carry):
        cols = pl.ds(pl.multiple_of(i * wide, wide), wide)
        normed = (tok[:, cols].astype(F32) * inv[...] * gain[:, cols]).astype(BF16)
        res = lax.dot_general(
            normed, cot[...], (((0,), (0,)), ((), ())), preferred_element_type=F32
        )
        res = (res * scale).astype(BF16)
        group = res.shape[1] // (2 * QUAD)
        for b in range(2):
            for j in range(NJ):
                lo = b * BLK + j * SUB
                for k in range(QUAD):
                    for cc in range(2):
                        col = (k * 2 + cc) * group
                        part[cc, j, k, i * 2 + b] = res[lo:lo + SUB, col:col + group]
        return carry


    hb = nblk // 2

    def d_copy(j, i):
        blocks = pl.ds(i * hb, hb)
        return rdma(
            part.at[oc, j, :, blocks], drecv.at[j, :, blocks], d_s.at[j, i], d_r.at[j, i], partner
        )

    for i in range(2):
        lax.fori_loop(i * hb // 2, (i + 1) * hb // 2, term, 0)
        for j in range(NJ):
            d_copy(j, i).start()

    def add_to(dst, src, count):
        step = 8

        def body(i, carry):
            sl = pl.ds(i * step, step)
            dst[sl] = (dst[sl].astype(F32) + src[sl].astype(F32)).astype(BF16)
            return carry

        lax.fori_loop(0, count // step, body, 0)

    def first_hop(j):
        near, dev = (xq, xdev) if j % 2 == 0 else (yq, ydev)
        return (
            rdma(part.at[c, j, near], r1.at[j, 0], r1_s.at[j, 0], r1_r.at[j, 0], dev),
            rdma(part.at[c, j, dq], r1.at[j, 1], r1_s.at[j, 1], r1_r.at[j, 1], dev),
        )

    def second_hop(j):
        far, dev = (yq, ydev) if j % 2 == 0 else (xq, xdev)
        return rdma(part.at[c, j, far], r2.at[j], r2_s.at[j], r2_r.at[j], dev)

    def core_sum(j):
        for i in range(2):
            d_copy(j, i).wait()
        for k in range(QUAD):
            add_to(part.at[c, j, k], drecv.at[j, k], nblk)

    def first_send(j):
        hops = first_hop(j)
        hops[1].start()
        hops[0].start()

    def second_send(j):
        hops = first_hop(j)
        far = yq if j % 2 == 0 else xq
        hops[1].wait_recv()
        add_to(part.at[c, j, far], r1.at[j, 1], nblk)
        second_hop(j).start()
        hops[0].wait_recv()
        add_to(part.at[c, j, quad], r1.at[j, 0], nblk)

    per_plane = 2 * cap

    def z_copy(buf, ss, rs, j, q, dev):
        return rdma(slots.at[j, q], buf.at[j, q], ss.at[j, q], rs.at[j, q], dev)

    def up_copy(j, q):
        return z_copy(zup, zu_s, zu_r, j, q, updev)

    def dn_copy(j, q):
        return z_copy(zdn, zd_s, zd_r, j, q, dndev)

    def place(j):
        second_hop(j).wait_recv()
        add_to(part.at[c, j, quad], r2.at[j], nblk)

        def body(i, carry):
            for u in range(per_plane):
                b = bos[i * per_plane + u]
                val = part[c, j, quad, jnp.maximum(b, 0)]
                slots[j, i, u] = jnp.where(b >= 0, val.astype(F32), 0.0).astype(BF16)
            return carry

        lax.fori_loop(0, planes, body, 0)

    def z_start(chunks):
        for t in range(planes - 1):
            for j in chunks:
                @pl.when(z == 0)
                def _():
                    up_copy(j, planes - 1 - t).start()

                @pl.when(z == planes - 1)
                def _():
                    dn_copy(j, t).start()

    def z_step(j, t):
        qu = planes - 1 - t

        @pl.when(has_dn & (z < qu))
        def _():
            up_copy(j, qu).wait_recv()
            add_to(slots.at[j, qu], zup.at[j, qu], per_plane)
            up_copy(j, qu).start()

        @pl.when(has_up & (z > t))
        def _():
            dn_copy(j, t).wait_recv()
            add_to(slots.at[j, t], zdn.at[j, t], per_plane)
            dn_copy(j, t).start()

    my_id = quad * 2 + c

    def f_copies(j):
        out = []
        for n, dev in enumerate(plane):
            cc = oc if n % 2 == 0 else c
            out.append(
                rdma(
                    fin.at[j, pl.ds(cc * cap, cap)], frecv.at[my_id, j],
                    f_s.at[j, n], f_r.at[j, my_id], dev,
                )
            )
        return out

    def z_end(j):
        @pl.when(has_dn)
        def _():
            up_copy(j, z).wait_recv()
            add_to(slots.at[j, z], zup.at[j, z], per_plane)

        @pl.when(has_up)
        def _():
            dn_copy(j, z).wait_recv()
            add_to(slots.at[j, z], zdn.at[j, z], per_plane)

        fin[j] = slots[j, z]
        frecv[my_id, j] = slots[j, z, pl.ds(c * cap, cap)]
        for cp in f_copies(j):
            cp.start()

    grp = 4
    gw = grp * BLK

    def weight_group(g):
        return jnp.concatenate([whole[slot_of[g * grp + i]] for i in range(grp)], axis=0)

    def fwd_body(g, carry):
        cols = pl.ds(pl.multiple_of(g * gw, gw), gw)
        normed = (tok[:, cols].astype(F32) * inv[...] * gain[:, cols]).astype(BF16)
        fwd[...] += jnp.dot(normed, weight_group(g), preferred_element_type=F32)
        return carry

    def bwd_body(g, carry):
        cols = pl.ds(pl.multiple_of(g * gw, gw), gw)
        grad = lax.dot_general(
            cot[...], weight_group(g), (((1,), (1,)), ((), ())), preferred_element_type=F32
        )
        values = tok[:, cols].astype(F32)
        tgrad[:, cols] = (grad * gain[:, cols] * inv[...] - values * coef[...]).astype(BF16)
        gst[0, :, cols] = jnp.sum(grad * values * inv[...], axis=0, keepdims=True) * scale
        return carry

    groups = nblk // grp
    cuts = [0, groups // 2, groups]

    def fwd_part(i):
        lax.fori_loop(cuts[i], cuts[i + 1], fwd_body, 0)

    def bwd_part(i):
        lax.fori_loop(cuts[i], cuts[i + 1], bwd_body, 0)

    def fwd_end():
        total = fwd[...]
        proj[...] = (total + bias[...]).astype(BF16)
        inner = jnp.sum(total * cot[...].astype(F32), axis=1, keepdims=True) / width
        coef[...] = inv[...] * inv[...] * inner

    def g_copy(n):
        dev = (partner, xdev, ydev)[n]
        return rdma(gst.at[n], grecv.at[n], g_s.at[n], g_r.at[n], dev)

    def g_step(n):
        g_copy(n).wait_recv()
        gst[n + 1] = gst[n] + grecv[n]
        if n < 2:
            g_copy(n + 1).start()

    def gz_copy(d):
        return rdma(gst.at[3], gz.at[z], gz_s.at[d - 1], gz_r.at[z], others[d - 1])

    def gz_got(d):
        q = (z + d) % planes
        return rdma(gst.at[3], gz.at[q], gz_s.at[d - 1], gz_r.at[q], others[d - 1])

    own_local.wait()
    fwd[...] = jnp.zeros_like(fwd)
    gst[0, :, width:] = jnp.sum(cot[...].astype(F32), axis=0, keepdims=True) * scale
    early = list(range(NJ // 2))
    late = list(range(NJ // 2, NJ))
    for j in early:
        core_sum(j)
        first_send(j)
    for j in late:
        core_sum(j)
    ag_arrive(1)
    for j in early:
        second_send(j)
    for j in late:
        first_send(j)
    for t in range(2, planes - 1):
        ag_side(t - 1)
        ag_arrive(t)
    for j in early:
        place(j)
    z_start(early)
    for j in early:
        z_step(j, 0)
    for j in late:
        second_send(j)
    for j in early:
        z_step(j, 1)
    ag_side(planes - 2)
    ag_arrive(planes - 1)
    for t in range(2, planes - 1):
        for j in early:
            z_step(j, t)
    for j in late:
        place(j)
    z_start(late)
    for j in early:
        z_end(j)
    ag_side(planes - 1)
    for t in range(1, planes):
        ag_finish(t)
    rdma(
        w, span(2 * z + oc, 0, cap), agp_s.at[0, z], agp_r.at[0, z], partner
    ).wait_recv()
    fwd_part(0)
    for j in late:
        z_step(j, 0)
    fwd_part(1)
    for t in range(1, planes - 1):
        for j in late:
            z_step(j, t)
    middle = has_up & has_dn

    @pl.when(middle)
    def _():
        for j in late:
            z_end(j)

    fwd_end()
    bwd_part(0)
    bwd_part(1)
    g_copy(0).start()

    @pl.when(jnp.logical_not(middle))
    def _():
        for j in late:
            z_end(j)

    def f_got(j, n):
        ids = [quad * 2 + oc]
        for q in (xq, yq, dq):
            ids += [q * 2 + c, q * 2 + oc]
        sender = ids[n]
        return rdma(
            fin.at[j, pl.ds(0, cap)], frecv.at[sender, j],
            f_s.at[j, n], f_r.at[j, sender], plane[n],
        )

    for j in range(NJ):
        for n in range(7):
            f_got(j, n).wait_recv()

        def body(u, carry):
            for n in range(8):
                wgrad[pl.ds(pl.multiple_of(u * BLK + j * SUB, SUB), SUB), n * BLK:(n + 1) * BLK] = (
                    frecv[n, j, u].astype(F32)
                )
            return carry

        lax.fori_loop(0, cap, body, 0)
        if j < 3:
            g_step(j)
        if j == 2:
            gz[z] = gst[3]
            for d in range(1, planes):
                gz_copy(d).start()

    for d in range(1, planes):
        gz_got(d).wait_recv()
    total = gz[0]
    for q in range(1, planes):
        total = total + gz[q]
    vec[...] = total
    for d in range(1, planes):
        gz_copy(d).wait_send()
    for n in range(3):
        g_copy(n).wait_send()

    for t in range(1, planes):
        ag_drain(t)
    own_partner.wait_send()
    for j in range(NJ):
        for cp in first_hop(j):
            cp.wait_send()
        second_hop(j).wait_send()
        for cp in f_copies(j):
            cp.wait_send()
        for t in range(planes - 1):
            @pl.when(z < planes - 1 - t)
            def _():
                up_copy(j, planes - 1 - t).wait_send()

            @pl.when(z > t)
            def _():
                dn_copy(j, t).wait_send()

    @pl.when(has_up)
    def _():
        own_z(0, updev).wait_send()

    @pl.when(has_dn)
    def _():
        own_z(1, dndev).wait_send()


def communicate(tokens, norm_gain, cotangent, key_bias, block_of_slot, block_slot, key_weight, scale):
    shard_count = lax.axis_size("shard")
    planes = shard_count // 2
    rows, cols = key_weight.shape
    cap = rows // BLK
    tok_count, width = tokens.shape
    nblk = width // BLK
    group = cols // (2 * QUAD)
    dma = pltpu.SemaphoreType.DMA
    vm = pltpu.VMEM
    return pl.pallas_call(
        functools.partial(comm_kernel, planes, cap, nblk, scale),
        out_shape=(
            jax.ShapeDtypeStruct((tok_count, cols), BF16),
            jax.ShapeDtypeStruct((tok_count, width), BF16),
            jax.ShapeDtypeStruct((rows, cols), F32),
            jax.ShapeDtypeStruct((1, width + cols), F32),
        ),
        in_specs=[
            pl.BlockSpec(memory_space=vm),
            pl.BlockSpec(memory_space=vm),
            pl.BlockSpec(memory_space=vm),
            pl.BlockSpec(memory_space=vm),
            pl.BlockSpec(memory_space=pltpu.SMEM),
            pl.BlockSpec(memory_space=pltpu.SMEM),
            pl.BlockSpec(memory_space=vm),
        ],
        out_specs=(pl.BlockSpec(memory_space=vm),) * 4,
        scratch_shapes=[
            vm((shard_count * cap, BLK, cols), BF16),
            vm((tok_count, 1), F32),
            vm((tok_count, 1), F32),
            vm((tok_count, cols), F32),
            vm((4, 1, width + cols), F32),
            vm((3, 1, width + cols), F32),
            vm((planes, 1, width + cols), F32),
            vm((2, NJ, QUAD, nblk, SUB, group), BF16),
            vm((NJ, QUAD, nblk, SUB, group), BF16),
            vm((NJ, 2, nblk, SUB, group), BF16),
            vm((NJ, nblk, SUB, group), BF16),
            vm((NJ, planes, 2 * cap, SUB, group), BF16),
            vm((NJ, planes, 2 * cap, SUB, group), BF16),
            vm((NJ, planes, 2 * cap, SUB, group), BF16),
            vm((NJ, 2 * cap, SUB, group), BF16),
            vm((2 * QUAD, NJ, cap, SUB, group), BF16),
            dma(()),
            dma((2, planes)), dma((planes,)),
            dma((planes,)), dma((planes,)),
            dma((planes,)), dma((planes,)),
            dma((4, planes)), dma((4, planes)),
            dma((NJ, 2)), dma((NJ, 2)),
            dma((NJ, 2)), dma((NJ, 2)),
            dma((NJ,)), dma((NJ,)),
            dma((NJ, planes)), dma((NJ, planes)),
            dma((NJ, planes)), dma((NJ, planes)),
            dma((NJ, 7)), dma((NJ, 8)),
            dma((3,)), dma((3,)),
            dma((planes,)), dma((planes,)),
        ],
        compiler_params=pltpu.CompilerParams(
            collective_id=0, has_side_effects=True, vmem_limit_bytes=67043328
        ),
    )(
        tokens, norm_gain[None, :], cotangent, key_bias[None, :], block_of_slot, block_slot,
        key_weight.reshape(cap, BLK, cols),
    )


def local(tokens, norm_gain, key_bias, key_weight, cotangent, block_slot):
    row_count, width = tokens.shape
    shard_count = lax.axis_size("shard")
    replicas = lax.axis_size("rep")
    cap = key_weight.shape[0] // BLK
    slot_total = shard_count * cap
    block_count = width // BLK
    grad_scale = float(row_count * shard_count * replicas) ** (-0.5)
    match = block_slot[None, :] == jnp.arange(slot_total, dtype=jnp.int32)[:, None]
    numbers = jnp.arange(1, block_count + 1, dtype=jnp.int32)[None, :]
    block_of_slot = jnp.sum(jnp.where(match, numbers, 0), axis=1) - 1
    projected, token_grad, weight_grad, vec = communicate(
        tokens, norm_gain, cotangent, key_bias, block_of_slot, block_slot, key_weight, grad_scale
    )
    if replicas > QUAD:
        groups = [list(range(i, replicas, QUAD)) for i in range(QUAD)]
        weight_grad, vec = lax.psum((weight_grad, vec), "rep", axis_index_groups=groups)
    return (projected, token_grad, weight_grad, vec[0, :width], vec[0, width:])


def solution(mesh):
    return jax.shard_map(
        local,
        mesh=mesh,
        in_specs=(
            P(("shard", "rep"), None),
            P(),
            P(),
            P("shard", None),
            P(("shard", "rep"), None),
            P(),
        ),
        out_specs=(
            P(("shard", "rep"), None),
            P(("shard", "rep"), None),
            P("shard", None),
            P(),
            P(),
        ),
        check_vma=False,
    )
```
